32 devices in a mesh: blk: 4 (over x, core), grp: 8 (over z, y).
Axes of the slice: x: 2, y: 2, z: 4, core: 2. Of those that a mesh axis runs over, the one named last changes fastest.
Arguments:
- features: float32 [49152, 256], P(('blk', 'grp')), may hold values from -6 to 6
- initial: bfloat16 [49152, 256], P(('blk', 'grp')), may hold values from -6 to 6
- history: bfloat16 [49152, 256], P(('blk', 'grp')), may hold values from -6 to 6
- weight: bfloat16 [256, 256], replicated, may hold values from -0.375 to 0.375
- column_ids: int32 [384, 16], P(('blk', 'grp')), may hold values from 0 to 23, as said below
- block_values: bfloat16 [384, 16, 128, 128], P(('blk', 'grp')), may hold values from -0.125 to 0.125
- group_table: int32 [4, 8, 8], P('blk'), may hold values from 0 to 11
- loop_table: int32 [8, 4, 4], P('grp'), may hold values from 0 to 11
Outputs:
- refreshed: float32 [49152, 256], P(('blk', 'grp'))
- inbox: float32 [49152, 256], P(('blk', 'grp'))
The draws below stay inside these ranges and needn't reach their ends.
Inputs may be any that keep to these rules, and one draw needn't show every extreme that they name: `column_ids`: among the 16 entries of the 12 row tiles of one device, every slot from 0 to 12 + 8 + 4 - 1 appears at least once.
All inputs are finite; a program needn't handle non-finite values.
Results may differ from the reference program's by a relative error of at most 0.004.
Values may be sent and summed in bfloat16 or wider, within the bound.
A program may use at most 128 MiB of HBM per device.

```python
import math
import jax
import jax.numpy as jnp
import numpy as np
from jax import lax

H = 256
TILE = 128
K = 16
BLK_DEV = 12
TILES = 384
NODES = 49152
N_BLK = 4
N_GRP = 8


def draw_column_ids(key, part):
    slots = BLK_DEV + N_GRP + N_BLK
    count = BLK_DEV * K
    device_count = N_BLK * N_GRP
    device_keys = jax.random.split(jax.random.fold_in(key, 7), device_count)

    def one_device(device_key):
        first_key, second_key = jax.random.split(device_key)
        extra = jax.random.randint(first_key, (count - slots,), 0, slots).astype(jnp.int32)
        base = jnp.concatenate([jnp.arange(slots, dtype=jnp.int32), extra])
        return jax.random.permutation(second_key, base).reshape(BLK_DEV, K)
    return jax.vmap(one_device)(device_keys).reshape(device_count * BLK_DEV, K).astype(jnp.int32)


def plant(result, stream_key, least, high):
    spot = [jax.random.randint(jax.random.fold_in(stream_key, axis), (), 0, length) for axis, length in enumerate(result.shape)]
    main_axis = result.shape.index(max(result.shape))
    next_to = spot[:main_axis] + [(spot[main_axis] + 1) % result.shape[main_axis]] + spot[main_axis + 1:]
    return result.at[tuple(spot)].set(least).at[tuple(next_to)].set(high)


def steps_of(own_key, dims, pieces, low, high):
    gain, own = 1.0, jax.random.fold_in(own_key, 6)
    for dim, shards_of in pieces:
        draws = jnp.exp(jax.random.uniform(jax.random.fold_in(own, dim), (shards_of,), jnp.float32, low / len(pieces), high / len(pieces)))
        gain = gain * jnp.repeat(draws, dims[dim] // shards_of).reshape([-1 if axis == dim else 1 for axis in range(len(dims))])
    return gain


def cumulative_ranks(number_of, skew):
    portions = [(1 << 20) // math.isqrt(rank ** skew) + 1 for rank in range(1, number_of + 1)]
    scale = 1 + sum(portions) // (1 << 30)
    return np.cumsum(np.array([max(1, weight // scale) for weight in portions]))


def skewed_ids(stream_key, extent, number_of, slope):
    grid = cumulative_ranks(number_of, slope)
    pick = jax.random.randint(jax.random.fold_in(stream_key, 1), extent, 0, int(grid[number_of - 1]))
    rank = jnp.searchsorted(jnp.asarray(grid, jnp.int32), pick, side="right")
    return jax.random.permutation(jax.random.fold_in(stream_key, 2), number_of)[rank].astype(jnp.int32)


def centred(key, shape, spread, limit, shards=(), kind=jnp.bfloat16):
    array = spread * jax.random.normal(key, shape, jnp.float32)
    if shards:
        array = array * steps_of(key, shape, shards, -0.22, 0.18)
    return jnp.clip(array, -limit, limit).astype(kind)


def setup_inputs(seed: int = 0) -> dict:
    seeds = jax.random.split(jax.random.key(seed), 9)
    features = centred(seeds[0], (NODES, H), 1.0, 6.0, ((0, 32),), jnp.float32)
    initial = centred(seeds[1], (NODES, H), 1.0, 6.0, ((0, 32),))
    history = centred(seeds[2], (NODES, H), 1.0, 6.0, ((0, 32),))
    weight = centred(seeds[3], (H, H), H ** -0.5, 0.375)
    column_ids = draw_column_ids(jax.random.fold_in(seeds[8], 71), 0)
    block_values = centred(seeds[5], (TILES, K, TILE, TILE), (TILE * K) ** -0.5, 0.125, ((0, 32),))
    group_table = plant(skewed_ids(seeds[6], (N_BLK, N_GRP, N_GRP), BLK_DEV, 2), jax.random.fold_in(seeds[6], 3), 0, BLK_DEV - 1).astype(jnp.int32)
    loop_table = plant(skewed_ids(seeds[7], (N_GRP, N_BLK, N_BLK), BLK_DEV, 2), jax.random.fold_in(seeds[7], 3), 0, BLK_DEV - 1).astype(jnp.int32)
    return {"features": features, "initial": initial, "history": history, "weight": weight, "column_ids": column_ids, "block_values": block_values, "group_table": group_table, "loop_table": loop_table}


teleport = 0.1
mapping_share = 0.5


def reference(features, initial, history, weight, column_ids, block_values, group_table, loop_table):
    device_count = N_BLK * N_GRP
    slots = BLK_DEV + N_GRP + N_BLK
    fresh_blocks = features.astype(jnp.bfloat16).reshape(device_count, BLK_DEV, TILE, H)
    stale_blocks = history.reshape(device_count, BLK_DEV, TILE, H)
    start_blocks = initial.reshape(device_count, BLK_DEV, TILE, H)
    columns = column_ids.reshape(device_count, BLK_DEV, K)
    values = block_values.reshape(device_count, BLK_DEV, K, TILE, TILE)
    group_range = jnp.arange(N_GRP, dtype=jnp.int32)
    loop_range = jnp.arange(N_BLK, dtype=jnp.int32)
    slot_range = jnp.arange(slots, dtype=jnp.int32)

    def owners_of(device):
        loop_pos = device // N_GRP
        group_pos = device % N_GRP
        group_owner = loop_pos * N_GRP + group_range
        loop_owner = loop_range * N_GRP + group_pos
        group_block = group_table[loop_pos, :, group_pos]
        loop_block = loop_table[group_pos, :, loop_pos]
        owner = jnp.concatenate([group_owner, loop_owner]).astype(jnp.int32)
        block = jnp.concatenate([group_block, loop_block]).astype(jnp.int32)
        return owner, block

    def one_device(device):
        owner, block = owners_of(device)
        pulled = stale_blocks[owner, block]
        sources = jnp.concatenate([fresh_blocks[device], pulled], axis=0)
        column_rows = columns[device]
        picked = sources[column_rows].astype(jnp.float32)
        tile_values = values[device].astype(jnp.float32)
        gathered = jnp.einsum('tkij,tkjh->tih', tile_values, picked)
        start = start_blocks[device].astype(jnp.float32)
        mixed = ((1.0 - teleport) * gathered + teleport * start).astype(jnp.bfloat16).reshape(BLK_DEV * TILE, H)
        product = jnp.dot(mixed, weight, preferred_element_type=jnp.float32)
        refreshed = jax.nn.relu((1.0 - mapping_share) * mixed.astype(jnp.float32) + mapping_share * product)
        outgoing = refreshed.astype(jnp.bfloat16).reshape(BLK_DEV, TILE, H).astype(jnp.float32)
        each = jnp.einsum('tkij,tih->tkjh', tile_values, outgoing)
        selector = (column_rows[:, :, None] == slot_range[None, None, :]).astype(jnp.float32)
        messages = jnp.einsum('tks,tkjh->sjh', selector, each, precision=lax.Precision.HIGHEST)
        return refreshed, messages[BLK_DEV:].astype(jnp.bfloat16)

    device_ids = jnp.arange(device_count, dtype=jnp.int32)
    refreshed, messages = lax.map(one_device, device_ids)
    owner, block = jax.vmap(owners_of)(device_ids)
    targets = (owner * BLK_DEV + block).reshape(-1).astype(jnp.int32)
    inbox = jnp.zeros((device_count * BLK_DEV, TILE, H), jnp.float32)
    inbox = inbox.at[targets].add(messages.reshape(-1, TILE, H).astype(jnp.float32))
    return refreshed.reshape(NODES, H), inbox.reshape(NODES, H)
```

```python
import functools

import jax
import jax.numpy as jnp
from jax import lax
from jax.experimental import pallas as pl
from jax.experimental.pallas import tpu as pltpu
from jax.sharding import PartitionSpec as P

teleport = 0.1
mapping_share = 0.5
MAIN_LIMIT = 44 * 1024 * 1024
DELIVER_LIMIT = 6 * 1024 * 1024
MESH = pl.DeviceIdType.MESH
GATHER_UNROLL = 12
REFRESH_UNROLL = 12
MESSAGE_UNROLL = 32
LEAD = 0

PULL_FAR = False
MAIL_FAR = True


def row_of(size):
    row = 1
    while size % (2 * row) == 0 and 4 * row * row <= size:
        row *= 2
    return row


def along(position, size, far):
    row = row_of(size)
    lines = size // row
    line, spot = lax.div(position, row), lax.rem(position, row)
    found = []
    for n in range(1, lines):
        up = lines - n if far else line + n
        down = line + n - lines if far else lines - 1 - n
        there = jnp.where(line + n < lines, up, down)
        found += [there * row + lax.rem(spot + j, row) for j in range(row)]
    beside = [line * row + lax.rem(spot + j, row) for j in range(1, row)]
    return found + beside if far else beside + found


def slot_plan(ids_ref, plan, tiles, entries, remote, pairs):
    count = tiles * entries
    width = plan.shape[1]
    iota = lambda shape, axis: lax.broadcasted_iota(jnp.int32, shape, axis)
    total = lambda value, axis: jnp.sum(value, axis=axis, keepdims=True)
    lane = iota((1, count), 1)
    row = jnp.zeros((1, count), jnp.int32)
    for t in range(tiles):
        for k in range(entries):
            row = jnp.where(lane == t * entries + k, ids_ref[t, k] - tiles, row)
    down, across = iota((count, count), 0), iota((count, count), 1)
    column = total(jnp.where(down == across, row, 0), 1)
    even = lambda value: value + lax.rem(value, 2)
    sizes_row = even(total((column == iota((count, remote), 1)).astype(jnp.int32), 0))
    sizes_column = even(total((row == iota((remote, count), 0)).astype(jnp.int32), 1))
    low, high = iota((remote, remote), 0), iota((remote, remote), 1)
    first_row = total(jnp.where(low < high, sizes_column, 0), 0)
    first_column = total(jnp.where(high < low, sizes_row, 0), 1)
    before = total(jnp.where(iota((count, remote), 1) < column, sizes_row, 0), 1)
    rank = total(((column == row) & (across < down)).astype(jnp.int32), 1)
    place = jnp.where(column >= 0, before + rank, -1)
    seat = iota((count, width), 1)
    entry = total(jnp.where(place == seat, iota((count, width), 0) - count, 0), 0) + count
    halves = lax.shift_right_logical(first_column, 1)
    keep = 1 - total((halves == iota((remote, width), 1)).astype(jnp.int32), 0)
    plan[0:1, :] = entry
    plan[1:2, :] = keep
    last = jnp.maximum(lax.shift_right_logical(first_row + sizes_row, 1) - 1, 0)
    plan[2:3, 0:remote] = last


def kernel(
    sizes,
    ids_far,
    group_far,
    loop_far,
    features_ref,
    initial_ref,
    history_ref,
    weight_ref,
    values_ref,
    refreshed_ref,
    mail_ref,
    hist,
    feat,
    start,
    wgt,
    vals,
    turned,
    sources,
    outbox,
    fresh,
    outgoing,
    mixture,
    running,
    letters,
    plan_rows,
    plan,
    load_sem,
    tile_sem,
    store_sem,
    send_sem,
    recv_sem,
    mail_send,
    mail_recv,
    own_sem,
    plan_sem,
    ids_ref,
    group_ref,
    loop_ref,
    table_sem,
    go_sem,
):
    group, loop, tiles, entries, edge, hidden, pairs = sizes
    remote = group + loop
    group_pos = lax.axis_index("grp")
    loop_pos = lax.axis_index("blk")

    loads = [
        pltpu.make_async_copy(history_ref, hist, load_sem.at[0]),
        pltpu.make_async_copy(features_ref, feat, load_sem.at[1]),
        pltpu.make_async_copy(values_ref, vals.at[pl.ds(0, tiles * entries)], load_sem.at[2]),
        pltpu.make_async_copy(initial_ref, start, load_sem.at[3]),
        pltpu.make_async_copy(weight_ref, wgt, load_sem.at[4]),
    ]
    tables = [
        pltpu.make_async_copy(group_far, group_ref, table_sem.at[0]),
        pltpu.make_async_copy(loop_far, loop_ref, table_sem.at[1]),
        pltpu.make_async_copy(ids_far, ids_ref, table_sem.at[2]),
    ]
    for load in tables + loads[:1]:
        load.start()

    everyone = [("grp", n) for n in along(group_pos, group, PULL_FAR)]
    everyone += [("blk", lax.rem(loop_pos + n, loop)) for n in range(1, loop)]
    posts = [("grp", n) for n in along(group_pos, group, MAIL_FAR)] + everyone[group - 1 :]
    slot_of = lambda axis, there: there if axis == "grp" else group + there
    mine_of = lambda axis: group_pos if axis == "grp" else group + loop_pos

    barrier = pltpu.get_barrier_semaphore()
    for axis, there in everyone:
        pl.semaphore_signal(barrier, inc=1, device_id={axis: there}, device_id_type=MESH)

    for load in tables:
        load.wait()
    loads[0].wait()
    for load in loads[1:]:
        load.start()
    for n in range(remote):
        outbox[n] = hist[group_ref[group_pos, n] if n < group else loop_ref[loop_pos, n - group]]
    pl.semaphore_wait(barrier, len(everyone))

    def pull(axis, there, arriving):
        slot, mine = slot_of(axis, there), mine_of(axis)
        return pltpu.make_async_remote_copy(
            src_ref=outbox.at[slot],
            dst_ref=sources.at[tiles + (slot if arriving else mine)],
            send_sem=send_sem.at[slot],
            recv_sem=recv_sem.at[slot if arriving else mine],
            device_id={axis: there},
            device_id_type=MESH,
        )

    for axis, there in everyone[group - 1 :]:
        pull(axis, there, False).start()

    def pull_group():
        for axis, there in everyone[: group - 1]:
            pull(axis, there, False).start()

    leads = lax.rem(loop_pos, 2) == LEAD
    takes_turns = loop % 2 == 0
    if takes_turns:
        pl.when(leads)(pull_group)
    else:
        pull_group()
    sources[tiles + group_pos] = outbox[group_pos]
    sources[tiles + group + loop_pos] = outbox[group + loop_pos]
    loads[1].wait()
    sources[pl.ds(0, tiles)] = feat[...].astype(jnp.bfloat16)

    slot_plan(ids_ref, plan_rows, tiles, entries, remote, pairs)
    ordered = pltpu.make_async_copy(plan_rows, plan, plan_sem)
    ordered.start()
    vals[tiles * entries] = jnp.zeros((edge, edge), jnp.bfloat16)
    loads[2].wait()
    ordered.wait()

    def turn(m, _):
        both = jnp.concatenate([vals[plan[0, 2 * m]], vals[plan[0, 2 * m + 1]]], axis=0)
        turned[m] = both.T
        return 0

    lax.fori_loop(0, pairs, turn, 0, unroll=4)
    loads[3].wait()
    loads[4].wait()
    beside = loop_pos + 1 - 2 * lax.rem(loop_pos, 2)
    early = 3 * group // 8

    def hand_over():
        for axis, there in everyone[: group - 1 - early]:
            pull(axis, there, True).wait_send()
        pl.semaphore_signal(go_sem, inc=1, device_id={"blk": beside}, device_id_type=MESH)
        for axis, there in everyone[group - 1 - early : group - 1]:
            pull(axis, there, True).wait_send()

    if takes_turns:

        @pl.when(jnp.logical_not(leads))
        def _():
            pl.semaphore_wait(go_sem, 1)
            pull_group()

        hand_over()
    else:
        for axis, there in everyone[: group - 1]:
            pull(axis, there, True).wait_send()

    for axis, there in everyone:
        pull(axis, there, True).wait_recv()

    def gather(t, _):
        left = jnp.concatenate([vals[t * entries + k] for k in range(entries)], axis=1)
        right = jnp.concatenate([sources[ids_ref[t, k]] for k in range(entries)], axis=0)
        gathered = jnp.dot(left, right, preferred_element_type=jnp.float32)
        mixture[t] = (
            (1.0 - teleport) * gathered + teleport * start[t].astype(jnp.float32)
        ).astype(jnp.bfloat16)
        return 0

    lax.fori_loop(0, tiles, gather, 0, unroll=GATHER_UNROLL)

    def refresh(t, _):
        mixed = mixture[t]
        product = jnp.dot(mixed, wgt[...], preferred_element_type=jnp.float32)
        value = jnp.maximum(
            (1.0 - mapping_share) * mixed.astype(jnp.float32) + mapping_share * product, 0.0
        )
        fresh[t] = value
        outgoing[t] = value.astype(jnp.bfloat16)
        return 0

    lax.fori_loop(0, tiles, refresh, 0, unroll=REFRESH_UNROLL)
    store = pltpu.make_async_copy(fresh, refreshed_ref, store_sem)
    store.start()

    def gather_message(m, total):
        one = jnp.minimum(lax.div(plan[0, 2 * m], entries), tiles - 1)
        two = jnp.minimum(lax.div(plan[0, 2 * m + 1], entries), tiles - 1)
        right = jnp.concatenate([outgoing[one], outgoing[two]], axis=0)
        part = jnp.dot(turned[m], right, preferred_element_type=jnp.float32)
        total = jnp.where(plan[1, m] > 0, total, 0.0) + part
        running[m] = total.astype(jnp.bfloat16)
        return total

    lax.fori_loop(
        0, pairs, gather_message, jnp.zeros((edge, hidden), jnp.float32), unroll=MESSAGE_UNROLL
    )

    def mail(axis, there, arriving):
        slot, mine = slot_of(axis, there), mine_of(axis)
        return pltpu.make_async_remote_copy(
            src_ref=letters.at[slot],
            dst_ref=mail_ref.at[slot if arriving else mine],
            send_sem=mail_send.at[slot],
            recv_sem=mail_recv.at[slot if arriving else mine],
            device_id={axis: there},
            device_id_type=MESH,
        )

    for slot in range(remote):
        letters[slot] = running[plan[2, slot]]
    if takes_turns:

        @pl.when(leads)
        def _():
            pl.semaphore_wait(go_sem, 1)

    for axis, there in posts:
        mail(axis, there, False).start()
    own = [
        pltpu.make_async_copy(letters.at[slot], mail_ref.at[slot], own_sem.at[n])
        for n, slot in enumerate((group_pos, group + loop_pos))
    ]
    for copy in own:
        copy.start()
    for axis, there in everyone[group - 1 :]:
        pull(axis, there, True).wait_send()

    for copy in own:
        copy.wait()
    store.wait()
    for axis, there in everyone:
        mail(axis, there, True).wait()


def deliver(
    sizes, group_far, loop_far, fresh_ref, mail_ref, refreshed_ref, inbox_ref, sums, out_sem,
    group_ref, loop_ref, table_sem,
):
    group, loop, tiles = sizes
    group_pos = lax.axis_index("grp")
    loop_pos = lax.axis_index("blk")
    tables = [
        pltpu.make_async_copy(group_far, group_ref, table_sem.at[0]),
        pltpu.make_async_copy(loop_far, loop_ref, table_sem.at[1]),
    ]
    for load in tables:
        load.start()
    put_fresh = pltpu.make_async_copy(fresh_ref, refreshed_ref, out_sem.at[1])
    put_fresh.start()
    sums[...] = jnp.zeros_like(sums)
    for load in tables:
        load.wait()
    for n in range(group + loop):
        block = group_ref[group_pos, n] if n < group else loop_ref[loop_pos, n - group]
        sums[block] = sums[block] + mail_ref[n].astype(jnp.float32)
    put_sums = pltpu.make_async_copy(sums, inbox_ref, out_sem.at[0])
    put_sums.start()
    put_sums.wait()
    put_fresh.wait()


def body(features, initial, history, weight, column_ids, block_values, group_table, loop_table):
    group = lax.axis_size("grp")
    loop = lax.axis_size("blk")
    tiles, entries = column_ids.shape
    edge = block_values.shape[2]
    hidden = features.shape[1]
    remote = group + loop
    count = tiles * entries
    pairs = (count - tiles + remote) // 2
    pairs = -(-pairs // MESSAGE_UNROLL) * MESSAGE_UNROLL
    width = -(-2 * pairs // 128) * 128
    bf16, f32 = jnp.bfloat16, jnp.float32
    smem = pl.BlockSpec(memory_space=pltpu.SMEM)
    far = pl.BlockSpec(memory_space=pltpu.HBM)
    hbm = pl.BlockSpec(memory_space=pl.ANY)
    block = (tiles, edge, hidden)
    dma = pltpu.SemaphoreType.DMA
    refreshed, mail = pl.pallas_call(
        functools.partial(kernel, (group, loop, tiles, entries, edge, hidden, pairs)),
        out_shape=(
            jax.ShapeDtypeStruct(block, f32),
            jax.ShapeDtypeStruct((remote, edge, hidden), bf16),
        ),
        in_specs=[far] * 8,
        out_specs=(hbm, hbm),
        scratch_shapes=[
            pltpu.VMEM(block, bf16),
            pltpu.VMEM(block, f32),
            pltpu.VMEM(block, bf16),
            pltpu.VMEM((hidden, hidden), bf16),
            pltpu.VMEM((count + 1, edge, edge), bf16),
            pltpu.VMEM((pairs, edge, 2 * edge), bf16),
            pltpu.VMEM((tiles + remote, edge, hidden), bf16),
            pltpu.VMEM((remote, edge, hidden), bf16),
            pltpu.VMEM(block, f32),
            pltpu.VMEM(block, bf16),
            pltpu.VMEM(block, bf16),
            pltpu.VMEM((pairs, edge, hidden), bf16),
            pltpu.VMEM((remote, edge, hidden), bf16),
            pltpu.VMEM((8, width), jnp.int32),
            pltpu.SMEM((8, width), jnp.int32),
            dma((5,)),
            dma((1,)),
            dma,
            dma((remote,)),
            dma((remote,)),
            dma((remote,)),
            dma((remote,)),
            dma((2,)),
            dma,
            pltpu.SMEM((tiles, entries), jnp.int32),
            pltpu.SMEM((group, group), jnp.int32),
            pltpu.SMEM((loop, loop), jnp.int32),
            dma((3,)),
            pltpu.SemaphoreType.REGULAR,
        ],
        compiler_params=pltpu.CompilerParams(
            collective_id=0, has_side_effects=True, vmem_limit_bytes=MAIN_LIMIT
        ),
    )(
        *[
            pltpu.with_memory_space_constraint(x, pltpu.HBM)
            for x in (
                column_ids,
                group_table[0],
                loop_table[0],
                features.reshape(block),
                initial.reshape(block),
                history.reshape(block),
                weight,
                block_values.reshape(count, edge, edge),
            )
        ],
    )
    refreshed, inbox = pl.pallas_call(
        functools.partial(deliver, (group, loop, tiles)),
        out_shape=(jax.ShapeDtypeStruct(block, f32), jax.ShapeDtypeStruct(block, f32)),
        in_specs=[far] * 2 + [pl.BlockSpec(memory_space=pltpu.VMEM)] * 2,
        out_specs=(hbm, hbm),
        scratch_shapes=[
            pltpu.VMEM(block, f32),
            dma((2,)),
            pltpu.SMEM((group, group), jnp.int32),
            pltpu.SMEM((loop, loop), jnp.int32),
            dma((2,)),
        ],
        compiler_params=pltpu.CompilerParams(vmem_limit_bytes=DELIVER_LIMIT),
    )(
        pltpu.with_memory_space_constraint(group_table[0], pltpu.HBM),
        pltpu.with_memory_space_constraint(loop_table[0], pltpu.HBM),
        refreshed,
        mail,
    )
    return (refreshed.reshape(tiles * edge, hidden), inbox.reshape(tiles * edge, hidden))


def solution(mesh):
    in_specs = (
        P(("blk", "grp"), None),
        P(("blk", "grp"), None),
        P(("blk", "grp"), None),
        P(),
        P(("blk", "grp"), None),
        P(("blk", "grp"), None, None, None),
        P("blk", None, None),
        P("grp", None, None),
    )
    out_specs = (P(("blk", "grp"), None), P(("blk", "grp"), None))
    return jax.shard_map(body, mesh=mesh, in_specs=in_specs, out_specs=out_specs, check_vma=False)
```

```python
import functools

import jax
import jax.numpy as jnp
from jax import lax
from jax.experimental import pallas as pl
from jax.experimental.pallas import tpu as pltpu
from jax.sharding import PartitionSpec as P

teleport = 0.1
mapping_share = 0.5
MAIN_LIMIT = 44 * 1024 * 1024
DELIVER_LIMIT = 6 * 1024 * 1024
MESH = pl.DeviceIdType.MESH
GATHER_UNROLL = 12
REFRESH_UNROLL = 12
LEAD = 1
EARLY = 3
PULL = "near"
LEAD_MAIL = "far"
FOLLOW_MAIL = "far"


def row_of(size):
    row = 1
    while size % (2 * row) == 0 and 4 * row * row <= size:
        row *= 2
    return row


def along(position, size, order):
    row = row_of(size)
    lines = size // row
    line, spot = lax.div(position, row), lax.rem(position, row)
    last = lines - 1 - line
    found = []
    for n in range(1, lines):
        k = n - last
        if order == "near":
            up, down = line + n, line - k
        elif order == "far":
            up, down = lines - n, k - 1
        else:
            up = lines - 1 if n == 1 else line + n - 1
            down = jnp.where(k == 1, 0, line + 1 - k)
        there = jnp.where(n <= last, up, down)
        found += [there * row + lax.rem(spot + j, row) for j in range(row)]
    beside = [line * row + lax.rem(spot + j, row) for j in range(1, row)]
    return beside + found if order == "near" else found + beside


def slot_plan(ids_ref, plan, tiles, entries, remote, pairs):
    count = tiles * entries
    width = plan.shape[1]
    iota = lambda shape, axis: lax.broadcasted_iota(jnp.int32, shape, axis)
    total = lambda value, axis: jnp.sum(value, axis=axis, keepdims=True)
    lane = iota((1, count), 1)
    row = jnp.zeros((1, count), jnp.int32)
    for t in range(tiles):
        for k in range(entries):
            row = jnp.where(lane == t * entries + k, ids_ref[t, k] - tiles, row)
    down, across = iota((count, count), 0), iota((count, count), 1)
    column = total(jnp.where(down == across, row, 0), 1)
    even = lambda value: value + lax.rem(value, 2)
    sizes_row = even(total((column == iota((count, remote), 1)).astype(jnp.int32), 0))
    sizes_column = even(total((row == iota((remote, count), 0)).astype(jnp.int32), 1))
    low, high = iota((remote, remote), 0), iota((remote, remote), 1)
    first_row = total(jnp.where(low < high, sizes_column, 0), 0)
    first_column = total(jnp.where(high < low, sizes_row, 0), 1)
    before = total(jnp.where(iota((count, remote), 1) < column, sizes_row, 0), 1)
    rank = total(((column == row) & (across < down)).astype(jnp.int32), 1)
    place = jnp.where(column >= 0, before + rank, -1)
    seat = iota((count, width), 1)
    entry = total(jnp.where(place == seat, iota((count, width), 0) - count, 0), 0) + count
    halves = lax.shift_right_logical(first_column, 1)
    keep = 1 - total((halves == iota((remote, width), 1)).astype(jnp.int32), 0)
    plan[0:1, :] = entry
    plan[1:2, :] = keep
    last = jnp.maximum(lax.shift_right_logical(first_row + sizes_row, 1) - 1, 0)
    plan[2:3, 0:remote] = last


def kernel(
    sizes,
    ids_far,
    group_far,
    loop_far,
    features_ref,
    initial_ref,
    history_ref,
    weight_ref,
    values_ref,
    refreshed_ref,
    mail_ref,
    hist,
    feat,
    start,
    wgt,
    vals,
    turned,
    sources,
    outbox,
    fresh,
    outgoing,
    mixture,
    running,
    letters,
    plan_rows,
    plan,
    load_sem,
    tile_sem,
    store_sem,
    send_sem,
    recv_sem,
    mail_send,
    mail_recv,
    own_sem,
    plan_sem,
    ids_ref,
    group_ref,
    loop_ref,
    table_sem,
    go_sem,
):
    group, loop, tiles, entries, edge, hidden, pairs = sizes
    remote = group + loop
    group_pos = lax.axis_index("grp")
    loop_pos = lax.axis_index("blk")

    loads = [
        pltpu.make_async_copy(history_ref, hist, load_sem.at[0]),
        pltpu.make_async_copy(features_ref, feat, load_sem.at[1]),
        pltpu.make_async_copy(values_ref, vals.at[pl.ds(0, tiles * entries)], load_sem.at[2]),
        pltpu.make_async_copy(initial_ref, start, load_sem.at[3]),
        pltpu.make_async_copy(weight_ref, wgt, load_sem.at[4]),
    ]
    tables = [
        pltpu.make_async_copy(group_far, group_ref, table_sem.at[0]),
        pltpu.make_async_copy(loop_far, loop_ref, table_sem.at[1]),
        pltpu.make_async_copy(ids_far, ids_ref, table_sem.at[2]),
    ]
    for load in tables + loads[:1]:
        load.start()

    everyone = [("grp", n) for n in along(group_pos, group, PULL)]
    everyone += [("blk", lax.rem(loop_pos + n, loop)) for n in range(1, loop)]
    posts = [
        [("grp", n) for n in along(group_pos, group, order)] + everyone[group - 1 :]
        for order in (LEAD_MAIL, FOLLOW_MAIL)
    ]
    slot_of = lambda axis, there: there if axis == "grp" else group + there
    mine_of = lambda axis: group_pos if axis == "grp" else group + loop_pos

    barrier = pltpu.get_barrier_semaphore()
    for axis, there in everyone:
        pl.semaphore_signal(barrier, inc=1, device_id={axis: there}, device_id_type=MESH)

    for load in tables:
        load.wait()
    loads[0].wait()
    for load in loads[1:]:
        load.start()
    for n in range(remote):
        outbox[n] = hist[group_ref[group_pos, n] if n < group else loop_ref[loop_pos, n - group]]
    pl.semaphore_wait(barrier, len(everyone))

    def pull(axis, there, arriving):
        slot, mine = slot_of(axis, there), mine_of(axis)
        return pltpu.make_async_remote_copy(
            src_ref=outbox.at[slot],
            dst_ref=sources.at[tiles + (slot if arriving else mine)],
            send_sem=send_sem.at[slot],
            recv_sem=recv_sem.at[slot if arriving else mine],
            device_id={axis: there},
            device_id_type=MESH,
        )

    for axis, there in everyone[group - 1 :]:
        pull(axis, there, False).start()

    def pull_group():
        for axis, there in everyone[: group - 1]:
            pull(axis, there, False).start()

    leads = lax.rem(loop_pos, 2) == LEAD
    takes_turns = loop % 2 == 0
    if takes_turns:
        pl.when(leads)(pull_group)
    else:
        pull_group()
    sources[tiles + group_pos] = outbox[group_pos]
    sources[tiles + group + loop_pos] = outbox[group + loop_pos]
    loads[1].wait()
    sources[pl.ds(0, tiles)] = feat[...].astype(jnp.bfloat16)

    slot_plan(ids_ref, plan_rows, tiles, entries, remote, pairs)
    ordered = pltpu.make_async_copy(plan_rows, plan, plan_sem)
    ordered.start()
    vals[tiles * entries] = jnp.zeros((edge, edge), jnp.bfloat16)
    loads[2].wait()
    ordered.wait()

    def turn(m, _):
        both = jnp.concatenate([vals[plan[0, 2 * m]], vals[plan[0, 2 * m + 1]]], axis=0)
        turned[m] = both.T
        return 0

    lax.fori_loop(0, pairs, turn, 0, unroll=4)
    loads[3].wait()
    loads[4].wait()
    beside = loop_pos + 1 - 2 * lax.rem(loop_pos, 2)

    def hand_over(early):
        for axis, there in everyone[: group - 1 - early]:
            pull(axis, there, True).wait_send()
        pl.semaphore_signal(go_sem, inc=1, device_id={"blk": beside}, device_id_type=MESH)
        for axis, there in everyone[group - 1 - early : group - 1]:
            pull(axis, there, True).wait_send()

    if takes_turns:
        follows = jnp.logical_not(leads)

        @pl.when(follows)
        def _():
            pl.semaphore_wait(go_sem, 1)
            pull_group()

        hand_over(EARLY * group // 8)
    else:
        for axis, there in everyone[: group - 1]:
            pull(axis, there, True).wait_send()

    for axis, there in everyone:
        pull(axis, there, True).wait_recv()

    def gather(t, _):
        left = jnp.concatenate([vals[t * entries + k] for k in range(entries)], axis=1)
        right = jnp.concatenate([sources[ids_ref[t, k]] for k in range(entries)], axis=0)
        gathered = jnp.dot(left, right, preferred_element_type=jnp.float32)
        mixture[t] = (
            (1.0 - teleport) * gathered + teleport * start[t].astype(jnp.float32)
        ).astype(jnp.bfloat16)
        return 0

    lax.fori_loop(0, tiles, gather, 0, unroll=GATHER_UNROLL)

    def refresh(t, _):
        mixed = mixture[t]
        product = jnp.dot(mixed, wgt[...], preferred_element_type=jnp.float32)
        value = jnp.maximum(
            (1.0 - mapping_share) * mixed.astype(jnp.float32) + mapping_share * product, 0.0
        )
        fresh[t] = value
        outgoing[t] = value.astype(jnp.bfloat16)
        return 0

    lax.fori_loop(0, tiles, refresh, 0, unroll=REFRESH_UNROLL)
    store = pltpu.make_async_copy(fresh, refreshed_ref, store_sem)
    store.start()

    def gather_message(m, total):
        one = jnp.minimum(lax.div(plan[0, 2 * m], entries), tiles - 1)
        two = jnp.minimum(lax.div(plan[0, 2 * m + 1], entries), tiles - 1)
        right = jnp.concatenate([outgoing[one], outgoing[two]], axis=0)
        part = jnp.dot(turned[m], right, preferred_element_type=jnp.float32)
        total = jnp.where(plan[1, m] > 0, total, 0.0) + part
        running[m] = total.astype(jnp.bfloat16)
        return total

    lax.fori_loop(
        0, pairs, gather_message, jnp.zeros((edge, hidden), jnp.float32), unroll=pairs
    )

    def mail(axis, there, arriving):
        slot, mine = slot_of(axis, there), mine_of(axis)
        return pltpu.make_async_remote_copy(
            src_ref=letters.at[slot],
            dst_ref=mail_ref.at[slot if arriving else mine],
            send_sem=mail_send.at[slot],
            recv_sem=mail_recv.at[slot if arriving else mine],
            device_id={axis: there},
            device_id_type=MESH,
        )

    for slot in range(remote):
        letters[slot] = running[plan[2, slot]]
    def post(which):
        if which == 0 and takes_turns:
            pl.semaphore_wait(go_sem, 1)
        for axis, there in posts[which]:
            mail(axis, there, False).start()

    if takes_turns:
        pl.when(leads)(lambda: post(0))
        pl.when(follows)(lambda: post(1))
    else:
        post(0)
    own = [
        pltpu.make_async_copy(letters.at[slot], mail_ref.at[slot], own_sem.at[n])
        for n, slot in enumerate((group_pos, group + loop_pos))
    ]
    for copy in own:
        copy.start()
    for axis, there in everyone[group - 1 :]:
        pull(axis, there, True).wait_send()

    for copy in own:
        copy.wait()
    store.wait()
    for axis, there in everyone:
        mail(axis, there, True).wait()


def deliver(
    sizes, group_far, loop_far, fresh_ref, mail_ref, refreshed_ref, inbox_ref, sums, out_sem,
    group_ref, loop_ref, table_sem,
):
    group, loop, tiles = sizes
    group_pos = lax.axis_index("grp")
    loop_pos = lax.axis_index("blk")
    tables = [
        pltpu.make_async_copy(group_far, group_ref, table_sem.at[0]),
        pltpu.make_async_copy(loop_far, loop_ref, table_sem.at[1]),
    ]
    for load in tables:
        load.start()
    put_fresh = pltpu.make_async_copy(fresh_ref, refreshed_ref, out_sem.at[1])
    put_fresh.start()
    sums[...] = jnp.zeros_like(sums)
    for load in tables:
        load.wait()
    for n in range(group + loop):
        block = group_ref[group_pos, n] if n < group else loop_ref[loop_pos, n - group]
        sums[block] = sums[block] + mail_ref[n].astype(jnp.float32)
    put_sums = pltpu.make_async_copy(sums, inbox_ref, out_sem.at[0])
    put_sums.start()
    put_sums.wait()
    put_fresh.wait()


def body(features, initial, history, weight, column_ids, block_values, group_table, loop_table):
    group = lax.axis_size("grp")
    loop = lax.axis_size("blk")
    tiles, entries = column_ids.shape
    edge = block_values.shape[2]
    hidden = features.shape[1]
    remote = group + loop
    count = tiles * entries
    pairs = -(-(count - tiles + remote) // 8) * 4
    width = -(-2 * pairs // 128) * 128
    bf16, f32 = jnp.bfloat16, jnp.float32
    smem = pl.BlockSpec(memory_space=pltpu.SMEM)
    far = pl.BlockSpec(memory_space=pltpu.HBM)
    hbm = pl.BlockSpec(memory_space=pl.ANY)
    block = (tiles, edge, hidden)
    dma = pltpu.SemaphoreType.DMA
    refreshed, mail = pl.pallas_call(
        functools.partial(kernel, (group, loop, tiles, entries, edge, hidden, pairs)),
        out_shape=(
            jax.ShapeDtypeStruct(block, f32),
            jax.ShapeDtypeStruct((remote, edge, hidden), bf16),
        ),
        in_specs=[far] * 8,
        out_specs=(hbm, hbm),
        scratch_shapes=[
            pltpu.VMEM(block, bf16),
            pltpu.VMEM(block, f32),
            pltpu.VMEM(block, bf16),
            pltpu.VMEM((hidden, hidden), bf16),
            pltpu.VMEM((count + 1, edge, edge), bf16),
            pltpu.VMEM((pairs, edge, 2 * edge), bf16),
            pltpu.VMEM((tiles + remote, edge, hidden), bf16),
            pltpu.VMEM((remote, edge, hidden), bf16),
            pltpu.VMEM(block, f32),
            pltpu.VMEM(block, bf16),
            pltpu.VMEM(block, bf16),
            pltpu.VMEM((pairs, edge, hidden), bf16),
            pltpu.VMEM((remote, edge, hidden), bf16),
            pltpu.VMEM((8, width), jnp.int32),
            pltpu.SMEM((8, width), jnp.int32),
            dma((5,)),
            dma((1,)),
            dma,
            dma((remote,)),
            dma((remote,)),
            dma((remote,)),
            dma((remote,)),
            dma((2,)),
            dma,
            pltpu.SMEM((tiles, entries), jnp.int32),
            pltpu.SMEM((group, group), jnp.int32),
            pltpu.SMEM((loop, loop), jnp.int32),
            dma((3,)),
            pltpu.SemaphoreType.REGULAR,
        ],
        compiler_params=pltpu.CompilerParams(
            collective_id=0, has_side_effects=True, vmem_limit_bytes=MAIN_LIMIT
        ),
    )(
        *[
            pltpu.with_memory_space_constraint(x, pltpu.HBM)
            for x in (
                column_ids,
                group_table[0],
                loop_table[0],
                features.reshape(block),
                initial.reshape(block),
                history.reshape(block),
                weight,
                block_values.reshape(count, edge, edge),
            )
        ],
    )
    refreshed, inbox = pl.pallas_call(
        functools.partial(deliver, (group, loop, tiles)),
        out_shape=(jax.ShapeDtypeStruct(block, f32), jax.ShapeDtypeStruct(block, f32)),
        in_specs=[far] * 2 + [pl.BlockSpec(memory_space=pltpu.VMEM)] * 2,
        out_specs=(hbm, hbm),
        scratch_shapes=[
            pltpu.VMEM(block, f32),
            dma((2,)),
            pltpu.SMEM((group, group), jnp.int32),
            pltpu.SMEM((loop, loop), jnp.int32),
            dma((2,)),
        ],
        compiler_params=pltpu.CompilerParams(vmem_limit_bytes=DELIVER_LIMIT),
    )(
        pltpu.with_memory_space_constraint(group_table[0], pltpu.HBM),
        pltpu.with_memory_space_constraint(loop_table[0], pltpu.HBM),
        refreshed,
        mail,
    )
    return (refreshed.reshape(tiles * edge, hidden), inbox.reshape(tiles * edge, hidden))


def solution(mesh):
    in_specs = (
        P(("blk", "grp"), None),
        P(("blk", "grp"), None),
        P(("blk", "grp"), None),
        P(),
        P(("blk", "grp"), None),
        P(("blk", "grp"), None, None, None),
        P("blk", None, None),
        P("grp", None, None),
    )
    out_specs = (P(("blk", "grp"), None), P(("blk", "grp"), None))
    return jax.shard_map(body, mesh=mesh, in_specs=in_specs, out_specs=out_specs, check_vma=False)
```

```python
import functools

import jax
import jax.numpy as jnp
from jax import lax
from jax.experimental import pallas as pl
from jax.experimental.pallas import tpu as pltpu
from jax.sharding import PartitionSpec as P

teleport = 0.1
mapping_share = 0.5
MAIN_LIMIT = 44 * 1024 * 1024
DELIVER_LIMIT = 6 * 1024 * 1024
MESH = pl.DeviceIdType.MESH
GATHER_UNROLL = 12
REFRESH_UNROLL = 12
LEAD = 1
EARLY = 3
PULL = "near"
LEAD_MAIL = "far"
FOLLOW_MAIL = "far"


def row_of(size):
    row = 1
    while size % (2 * row) == 0 and 4 * row * row <= size:
        row *= 2
    return row


def along(position, size, order):
    row = row_of(size)
    lines = size // row
    line, spot = lax.div(position, row), lax.rem(position, row)
    last = lines - 1 - line
    found = []
    for n in range(1, lines):
        k = n - last
        if order == "near":
            up, down = line + n, line - k
        elif order == "far":
            up, down = lines - n, k - 1
        else:
            up = lines - 1 if n == 1 else line + n - 1
            down = jnp.where(k == 1, 0, line + 1 - k)
        there = jnp.where(n <= last, up, down)
        found += [there * row + lax.rem(spot + j, row) for j in range(row)]
    beside = [line * row + lax.rem(spot + j, row) for j in range(1, row)]
    return beside + found if order == "near" else found + beside


def slot_plan(ids_ref, plan, tiles, entries, remote, pairs):
    count = tiles * entries
    width = plan.shape[1]
    iota = lambda shape, axis: lax.broadcasted_iota(jnp.int32, shape, axis)
    total = lambda value, axis: jnp.sum(value, axis=axis, keepdims=True)
    lane = iota((1, count), 1)
    row = jnp.zeros((1, count), jnp.int32)
    for t in range(tiles):
        for k in range(entries):
            row = jnp.where(lane == t * entries + k, ids_ref[t, k] - tiles, row)
    down, across = iota((count, count), 0), iota((count, count), 1)
    column = total(jnp.where(down == across, row, 0), 1)
    even = lambda value: value + lax.rem(value, 2)
    sizes_row = even(total((column == iota((count, remote), 1)).astype(jnp.int32), 0))
    sizes_column = even(total((row == iota((remote, count), 0)).astype(jnp.int32), 1))
    low, high = iota((remote, remote), 0), iota((remote, remote), 1)
    first_row = total(jnp.where(low < high, sizes_column, 0), 0)
    first_column = total(jnp.where(high < low, sizes_row, 0), 1)
    before = total(jnp.where(iota((count, remote), 1) < column, sizes_row, 0), 1)
    rank = total(((column == row) & (across < down)).astype(jnp.int32), 1)
    place = jnp.where(column >= 0, before + rank, -1)
    seat = iota((count, width), 1)
    entry = total(jnp.where(place == seat, iota((count, width), 0) - count, 0), 0) + count
    halves = lax.shift_right_logical(first_column, 1)
    keep = 1 - total((halves == iota((remote, width), 1)).astype(jnp.int32), 0)
    plan[0:1, :] = entry
    plan[1:2, :] = keep
    last = jnp.maximum(lax.shift_right_logical(first_row + sizes_row, 1) - 1, 0)
    plan[2:3, 0:remote] = last


def kernel(
    sizes,
    ids_far,
    group_far,
    loop_far,
    features_ref,
    initial_ref,
    history_ref,
    weight_ref,
    values_ref,
    refreshed_ref,
    mail_ref,
    where_ref,
    hist,
    feat,
    start,
    wgt,
    vals,
    turned,
    sources,
    outbox,
    fresh,
    outgoing,
    mixture,
    running,
    letters,
    plan_rows,
    plan,
    load_sem,
    tile_sem,
    store_sem,
    send_sem,
    recv_sem,
    mail_send,
    mail_recv,
    own_sem,
    plan_sem,
    ids_ref,
    group_ref,
    loop_ref,
    table_sem,
    go_sem,
):
    group, loop, tiles, entries, edge, hidden, pairs = sizes
    remote = group + loop
    group_pos = lax.axis_index("grp")
    loop_pos = lax.axis_index("blk")

    loads = [
        pltpu.make_async_copy(history_ref, hist, load_sem.at[0]),
        pltpu.make_async_copy(features_ref, feat, load_sem.at[1]),
        pltpu.make_async_copy(values_ref, vals.at[pl.ds(0, tiles * entries)], load_sem.at[2]),
        pltpu.make_async_copy(initial_ref, start, load_sem.at[3]),
        pltpu.make_async_copy(weight_ref, wgt, load_sem.at[4]),
    ]
    tables = [
        pltpu.make_async_copy(group_far, group_ref, table_sem.at[0]),
        pltpu.make_async_copy(loop_far, loop_ref, table_sem.at[1]),
        pltpu.make_async_copy(ids_far, ids_ref, table_sem.at[2]),
    ]
    for load in tables + loads[:1]:
        load.start()

    everyone = [("grp", n) for n in along(group_pos, group, PULL)]
    everyone += [("blk", lax.rem(loop_pos + n, loop)) for n in range(1, loop)]
    posts = [
        [("grp", n) for n in along(group_pos, group, order)] + everyone[group - 1 :]
        for order in (LEAD_MAIL, FOLLOW_MAIL)
    ]
    slot_of = lambda axis, there: there if axis == "grp" else group + there
    mine_of = lambda axis: group_pos if axis == "grp" else group + loop_pos

    barrier = pltpu.get_barrier_semaphore()
    for axis, there in everyone:
        pl.semaphore_signal(barrier, inc=1, device_id={axis: there}, device_id_type=MESH)

    for load in tables:
        load.wait()
    loads[0].wait()
    for load in loads[1:]:
        load.start()
    for n in range(remote):
        outbox[n] = hist[group_ref[group_pos, n] if n < group else loop_ref[loop_pos, n - group]]
    pl.semaphore_wait(barrier, len(everyone))

    def pull(axis, there, arriving):
        slot, mine = slot_of(axis, there), mine_of(axis)
        return pltpu.make_async_remote_copy(
            src_ref=outbox.at[slot],
            dst_ref=sources.at[tiles + (slot if arriving else mine)],
            send_sem=send_sem.at[slot],
            recv_sem=recv_sem.at[slot if arriving else mine],
            device_id={axis: there},
            device_id_type=MESH,
        )

    for axis, there in everyone[group - 1 :]:
        pull(axis, there, False).start()

    def pull_group():
        for axis, there in everyone[: group - 1]:
            pull(axis, there, False).start()

    leads = lax.rem(loop_pos, 2) == LEAD
    takes_turns = loop % 2 == 0
    if takes_turns:
        pl.when(leads)(pull_group)
    else:
        pull_group()
    sources[tiles + group_pos] = outbox[group_pos]
    sources[tiles + group + loop_pos] = outbox[group + loop_pos]
    loads[1].wait()
    sources[pl.ds(0, tiles)] = feat[...].astype(jnp.bfloat16)

    slot_plan(ids_ref, plan_rows, tiles, entries, remote, pairs)
    lane = lax.broadcasted_iota(jnp.int32, where_ref.shape, 1)
    where = jnp.zeros(where_ref.shape, jnp.int32)
    for n in range(remote):
        block = group_ref[group_pos, n] if n < group else loop_ref[loop_pos, n - group]
        where = jnp.where(lane == n, block, where)
    where_ref[...] = where
    ordered = pltpu.make_async_copy(plan_rows, plan, plan_sem)
    ordered.start()
    vals[tiles * entries] = jnp.zeros((edge, edge), jnp.bfloat16)
    loads[2].wait()
    ordered.wait()

    def turn(m, _):
        both = jnp.concatenate([vals[plan[0, 2 * m]], vals[plan[0, 2 * m + 1]]], axis=0)
        turned[m] = both.T
        return 0

    lax.fori_loop(0, pairs, turn, 0, unroll=4)
    loads[3].wait()
    loads[4].wait()
    beside = loop_pos + 1 - 2 * lax.rem(loop_pos, 2)

    def hand_over(early):
        for axis, there in everyone[: group - 1 - early]:
            pull(axis, there, True).wait_send()
        pl.semaphore_signal(go_sem, inc=1, device_id={"blk": beside}, device_id_type=MESH)
        for axis, there in everyone[group - 1 - early : group - 1]:
            pull(axis, there, True).wait_send()

    if takes_turns:
        follows = jnp.logical_not(leads)

        @pl.when(follows)
        def _():
            pl.semaphore_wait(go_sem, 1)
            pull_group()

        hand_over(EARLY * group // 8)
    else:
        for axis, there in everyone[: group - 1]:
            pull(axis, there, True).wait_send()

    for axis, there in everyone:
        pull(axis, there, True).wait_recv()

    def gather(t, _):
        left = jnp.concatenate([vals[t * entries + k] for k in range(entries)], axis=1)
        right = jnp.concatenate([sources[ids_ref[t, k]] for k in range(entries)], axis=0)
        gathered = jnp.dot(left, right, preferred_element_type=jnp.float32)
        mixture[t] = (
            (1.0 - teleport) * gathered + teleport * start[t].astype(jnp.float32)
        ).astype(jnp.bfloat16)
        return 0

    lax.fori_loop(0, tiles, gather, 0, unroll=GATHER_UNROLL)

    def refresh(t, _):
        mixed = mixture[t]
        product = jnp.dot(mixed, wgt[...], preferred_element_type=jnp.float32)
        value = jnp.maximum(
            (1.0 - mapping_share) * mixed.astype(jnp.float32) + mapping_share * product, 0.0
        )
        fresh[t] = value
        outgoing[t] = value.astype(jnp.bfloat16)
        return 0

    lax.fori_loop(0, tiles, refresh, 0, unroll=REFRESH_UNROLL)
    store = pltpu.make_async_copy(fresh, refreshed_ref, store_sem)
    store.start()

    def gather_message(m, total):
        one = jnp.minimum(lax.div(plan[0, 2 * m], entries), tiles - 1)
        two = jnp.minimum(lax.div(plan[0, 2 * m + 1], entries), tiles - 1)
        right = jnp.concatenate([outgoing[one], outgoing[two]], axis=0)
        part = jnp.dot(turned[m], right, preferred_element_type=jnp.float32)
        total = jnp.where(plan[1, m] > 0, total, 0.0) + part
        running[m] = total.astype(jnp.bfloat16)
        return total

    lax.fori_loop(
        0, pairs, gather_message, jnp.zeros((edge, hidden), jnp.float32), unroll=pairs
    )

    def mail(axis, there, arriving):
        slot, mine = slot_of(axis, there), mine_of(axis)
        return pltpu.make_async_remote_copy(
            src_ref=letters.at[slot],
            dst_ref=mail_ref.at[slot if arriving else mine],
            send_sem=mail_send.at[slot],
            recv_sem=mail_recv.at[slot if arriving else mine],
            device_id={axis: there},
            device_id_type=MESH,
        )

    for slot in range(remote):
        letters[slot] = running[plan[2, slot]]
    def post(which):
        if which == 0 and takes_turns:
            pl.semaphore_wait(go_sem, 1)
        for axis, there in posts[which]:
            mail(axis, there, False).start()

    if takes_turns:
        pl.when(leads)(lambda: post(0))
        pl.when(follows)(lambda: post(1))
    else:
        post(0)
    own = [
        pltpu.make_async_copy(letters.at[slot], mail_ref.at[slot], own_sem.at[n])
        for n, slot in enumerate((group_pos, group + loop_pos))
    ]
    for copy in own:
        copy.start()
    for axis, there in everyone[group - 1 :]:
        pull(axis, there, True).wait_send()

    for copy in own:
        copy.wait()
    store.wait()
    for axis, there in everyone:
        mail(axis, there, True).wait()


def deliver(sizes, where_ref, fresh_ref, mail_ref, refreshed_ref, inbox_ref, sums, out_sem):
    remote = sizes
    put_fresh = pltpu.make_async_copy(fresh_ref, refreshed_ref, out_sem.at[1])
    put_fresh.start()
    row = where_ref[0:1, :]
    lane = lax.broadcasted_iota(jnp.int32, row.shape, 1)
    blocks = [jnp.sum(jnp.where(lane == n, row, 0)) for n in range(remote)]
    sums[...] = jnp.zeros_like(sums)
    for n, block in enumerate(blocks):
        sums[block] = sums[block] + mail_ref[n].astype(jnp.float32)
    put_sums = pltpu.make_async_copy(sums, inbox_ref, out_sem.at[0])
    put_sums.start()
    put_sums.wait()
    put_fresh.wait()


def body(features, initial, history, weight, column_ids, block_values, group_table, loop_table):
    group = lax.axis_size("grp")
    loop = lax.axis_size("blk")
    tiles, entries = column_ids.shape
    edge = block_values.shape[2]
    hidden = features.shape[1]
    remote = group + loop
    count = tiles * entries
    pairs = -(-(count - tiles + remote) // 8) * 4
    width = -(-2 * pairs // 128) * 128
    bf16, f32 = jnp.bfloat16, jnp.float32
    smem = pl.BlockSpec(memory_space=pltpu.SMEM)
    far = pl.BlockSpec(memory_space=pltpu.HBM)
    hbm = pl.BlockSpec(memory_space=pl.ANY)
    block = (tiles, edge, hidden)
    dma = pltpu.SemaphoreType.DMA
    refreshed, mail, where = pl.pallas_call(
        functools.partial(kernel, (group, loop, tiles, entries, edge, hidden, pairs)),
        out_shape=(
            jax.ShapeDtypeStruct(block, f32),
            jax.ShapeDtypeStruct((remote, edge, hidden), bf16),
            jax.ShapeDtypeStruct((8, -(-remote // 128) * 128), jnp.int32),
        ),
        in_specs=[far] * 8,
        out_specs=(hbm, hbm, pl.BlockSpec(memory_space=pltpu.VMEM)),
        scratch_shapes=[
            pltpu.VMEM(block, bf16),
            pltpu.VMEM(block, f32),
            pltpu.VMEM(block, bf16),
            pltpu.VMEM((hidden, hidden), bf16),
            pltpu.VMEM((count + 1, edge, edge), bf16),
            pltpu.VMEM((pairs, edge, 2 * edge), bf16),
            pltpu.VMEM((tiles + remote, edge, hidden), bf16),
            pltpu.VMEM((remote, edge, hidden), bf16),
            pltpu.VMEM(block, f32),
            pltpu.VMEM(block, bf16),
            pltpu.VMEM(block, bf16),
            pltpu.VMEM((pairs, edge, hidden), bf16),
            pltpu.VMEM((remote, edge, hidden), bf16),
            pltpu.VMEM((8, width), jnp.int32),
            pltpu.SMEM((8, width), jnp.int32),
            dma((5,)),
            dma((1,)),
            dma,
            dma((remote,)),
            dma((remote,)),
            dma((remote,)),
            dma((remote,)),
            dma((2,)),
            dma,
            pltpu.SMEM((tiles, entries), jnp.int32),
            pltpu.SMEM((group, group), jnp.int32),
            pltpu.SMEM((loop, loop), jnp.int32),
            dma((3,)),
            pltpu.SemaphoreType.REGULAR,
        ],
        compiler_params=pltpu.CompilerParams(
            collective_id=0, has_side_effects=True, vmem_limit_bytes=MAIN_LIMIT
        ),
    )(
        *[
            pltpu.with_memory_space_constraint(x, pltpu.HBM)
            for x in (
                column_ids,
                group_table[0],
                loop_table[0],
                features.reshape(block),
                initial.reshape(block),
                history.reshape(block),
                weight,
                block_values.reshape(count, edge, edge),
            )
        ],
    )
    refreshed, inbox = pl.pallas_call(
        functools.partial(deliver, remote),
        out_shape=(jax.ShapeDtypeStruct(block, f32), jax.ShapeDtypeStruct(block, f32)),
        in_specs=[pl.BlockSpec(memory_space=pltpu.VMEM)] * 3,
        out_specs=(hbm, hbm),
        scratch_shapes=[pltpu.VMEM(block, f32), dma((2,))],
        compiler_params=pltpu.CompilerParams(vmem_limit_bytes=DELIVER_LIMIT),
    )(where, refreshed, mail)
    return (refreshed.reshape(tiles * edge, hidden), inbox.reshape(tiles * edge, hidden))


def solution(mesh):
    in_specs = (
        P(("blk", "grp"), None),
        P(("blk", "grp"), None),
        P(("blk", "grp"), None),
        P(),
        P(("blk", "grp"), None),
        P(("blk", "grp"), None, None, None),
        P("blk", None, None),
        P("grp", None, None),
    )
    out_specs = (P(("blk", "grp"), None), P(("blk", "grp"), None))
    return jax.shard_map(body, mesh=mesh, in_specs=in_specs, out_specs=out_specs, check_vma=False)
```
